32 devices in a mesh: dp: 4 (over y, z), ep: 8 (over x, core).
Axes of the slice: x: 4, y: 2, z: 2, core: 2. Of those that a mesh axis runs over, the one named last changes fastest.
The devices are a block of a 4x4x8 slice.
Arguments:
- tokens: bfloat16 [2048, 2048], P(('dp', 'ep')), parts along dimension 0
- slot_ids: int32 [2048, 4, 32], P(('dp', 'ep')), parts along dimension 0
- request_rows: int32 [32, 8, 128], P(('dp', 'ep')), parts along dimension 0
- gate_vals: float32 [2048, 4, 32], P(('dp', 'ep')), parts along dimension 0
- grad_out: bfloat16 [2048, 2048], P(('dp', 'ep')), parts along dimension 0
- table_up: bfloat16 [16384, 2048], P('ep')
- table_down: bfloat16 [16384, 2048], P('ep')
Outputs:
- output 1: bfloat16 [2048, 2048], P(('dp', 'ep')), parts along dimension 0
- output 2: bfloat16 [2048, 2048], P(('dp', 'ep')), parts along dimension 0
- output 3: bfloat16 [65536, 2048], P(('dp', 'ep')), parts along dimension 0
- output 4: bfloat16 [65536, 2048], P(('dp', 'ep')), parts along dimension 0
There are 4 independent parts. The reference program is written for one: setup_inputs(seed, part) draws one part's arguments, and reference() takes and returns one part's arrays. A program takes and returns all parts, laid end to end along the dimension named above; an argument that names none is the same for every part.
All inputs are finite; a program needn't handle non-finite values.
Results may differ from the reference program's by a relative error of at most 0.00871581.
Values are sent between devices in bfloat16 or wider.
A program may use at most 768 MiB of HBM per device.

```python
import math
import jax
import jax.numpy as jnp
from jax import lax

TOKENS_DEV = 64
DISTINCT = 128
GROUP_SIZE = 8
EXPERTS = 16384
MODEL_DIM = 2048
NUM_HEADS = 4
TOP_K = 32


def draw_routing(route_key):
    rows_owner = EXPERTS // GROUP_SIZE
    sel_dev = TOKENS_DEV * NUM_HEADS * TOP_K
    slots_dev = GROUP_SIZE * DISTINCT
    hot_slots = max(1, DISTINCT // 8)
    sub_keys = jax.random.split(route_key, 9)
    owner_perm = jax.vmap(lambda one_key: jax.random.permutation(one_key, rows_owner))(jax.random.split(sub_keys[0], GROUP_SIZE))
    hot_first = jax.random.randint(sub_keys[1], (), 0, GROUP_SIZE)
    hot_second = (hot_first + 1 + jax.random.randint(sub_keys[2], (), 0, GROUP_SIZE - 1)) % GROUP_SIZE
    owner_iota = jnp.arange(GROUP_SIZE)
    hot_owner = (owner_iota == hot_first) | (owner_iota == hot_second)
    offsets = jax.random.randint(sub_keys[3], (GROUP_SIZE, GROUP_SIZE), 0, rows_owner)
    offsets = jnp.where(hot_owner[None, :], 0, offsets)
    window_cols = (offsets[:, :, None] + jnp.arange(DISTINCT)[None, None, :]) % rows_owner
    request_rows = owner_perm[owner_iota[None, :, None], window_cols]
    cover_rank = jax.vmap(lambda one_key: jax.random.permutation(one_key, sel_dev))(jax.random.split(sub_keys[4], GROUP_SIZE))
    hot_pick = jax.random.randint(sub_keys[5], (GROUP_SIZE, sel_dev), 0, 2) == 0
    hot_side = jnp.where(jax.random.randint(sub_keys[6], (GROUP_SIZE, sel_dev), 0, 2) == 0, hot_first, hot_second)
    hot_slot = hot_side * DISTINCT + jax.random.randint(sub_keys[7], (GROUP_SIZE, sel_dev), 0, hot_slots)
    cold_slot = jax.random.randint(sub_keys[8], (GROUP_SIZE, sel_dev), 0, slots_dev)
    slot_ids = jnp.where(cover_rank < slots_dev, cover_rank, jnp.where(hot_pick, hot_slot, cold_slot))
    slot_ids = slot_ids.reshape(GROUP_SIZE * TOKENS_DEV, NUM_HEADS, TOP_K).astype(jnp.int32)
    return slot_ids, request_rows.astype(jnp.int32)


def setup_inputs(seed: int = 0, part: int = 0) -> dict:
    part_key = jax.random.fold_in(jax.random.key(seed), part)
    key_tok, key_grad, key_gate, key_route = jax.random.split(part_key, 4)
    key_up, key_down = jax.random.split(jax.random.key(seed + 1), 2)
    n_tok = GROUP_SIZE * TOKENS_DEV
    sel_tok = NUM_HEADS * TOP_K
    tokens = jax.random.normal(key_tok, (n_tok, MODEL_DIM), jnp.float32)
    grad_out = jax.random.normal(key_grad, (n_tok, MODEL_DIM), jnp.float32)
    gate_vals = jax.random.uniform(key_gate, (n_tok, NUM_HEADS, TOP_K), jnp.float32, 0.25, 1.75)
    table_up = jax.random.normal(key_up, (EXPERTS, MODEL_DIM), jnp.float32) * MODEL_DIM ** -0.5
    table_down = jax.random.normal(key_down, (EXPERTS, MODEL_DIM), jnp.float32) * sel_tok ** -0.5
    slot_ids, request_rows = draw_routing(key_route)
    return dict(tokens=tokens.astype(jnp.bfloat16), slot_ids=slot_ids, request_rows=request_rows, gate_vals=gate_vals, grad_out=grad_out.astype(jnp.bfloat16), table_up=table_up.astype(jnp.bfloat16), table_down=table_down.astype(jnp.bfloat16))


def gelu_pair(pre_act):
    normal_cdf = 0.5 * (1.0 + lax.erf(pre_act * (2.0 ** -0.5)))
    normal_pdf = jnp.exp(-0.5 * pre_act * pre_act) * ((2.0 * math.pi) ** -0.5)
    return pre_act * normal_cdf, normal_cdf + pre_act * normal_pdf


def reference(tokens, slot_ids, request_rows, gate_vals, grad_out, table_up, table_down):
    n_tok = GROUP_SIZE * TOKENS_DEV
    sel_tok = NUM_HEADS * TOP_K
    rows_owner = EXPERTS // GROUP_SIZE
    slot_flat = slot_ids.reshape(n_tok, sel_tok)
    dev_idx = jnp.arange(n_tok)[:, None] // TOKENS_DEV
    owner_idx = slot_flat // DISTINCT
    expert_ids = owner_idx * rows_owner + request_rows[dev_idx, owner_idx, slot_flat % DISTINCT]
    cap_tokens = max(1, 2 ** 23 // (sel_tok * MODEL_DIM))
    block_tok = math.gcd(n_tok, 2 ** int(math.log2(cap_tokens)))
    n_blocks = n_tok // block_tok

    def scan_step(acc_pair, block_in):
        acc_up, acc_down = acc_pair
        x_blk, id_blk, gate_blk, dy_blk = block_in
        x_wide = x_blk.astype(jnp.float32)
        dy_wide = dy_blk.astype(jnp.float32)
        up_rows = table_up[id_blk].astype(jnp.float32)
        down_rows = table_down[id_blk].astype(jnp.float32)
        pre_act = jnp.einsum('bsd,bd->bs', up_rows, x_wide)
        act_val, slope_val = gelu_pair(pre_act)
        w_out = (gate_blk * act_val).astype(jnp.bfloat16).astype(jnp.float32)
        y_blk = jnp.einsum('bs,bsd->bd', w_out, down_rows)
        back_dot = jnp.einsum('bsd,bd->bs', down_rows, dy_wide)
        coef_val = (gate_blk * slope_val * back_dot).astype(jnp.bfloat16).astype(jnp.float32)
        dx_blk = jnp.einsum('bs,bsd->bd', coef_val, up_rows)
        flat_ids = id_blk.reshape(-1)
        acc_up = acc_up.at[flat_ids].add((coef_val[:, :, None] * x_wide[:, None, :]).reshape(-1, MODEL_DIM))
        acc_down = acc_down.at[flat_ids].add((w_out[:, :, None] * dy_wide[:, None, :]).reshape(-1, MODEL_DIM))
        return (acc_up, acc_down), (y_blk, dx_blk)

    zero_acc = jnp.zeros((EXPERTS, MODEL_DIM), jnp.float32)
    blocks_in = (tokens.reshape(n_blocks, block_tok, MODEL_DIM), expert_ids.reshape(n_blocks, block_tok, sel_tok), gate_vals.reshape(n_blocks, block_tok, sel_tok), grad_out.reshape(n_blocks, block_tok, MODEL_DIM))
    (acc_up, acc_down), (y_all, dx_all) = lax.scan(scan_step, (zero_acc, zero_acc), blocks_in)
    out_tokens = y_all.reshape(n_tok, MODEL_DIM).astype(jnp.bfloat16)
    grad_tokens = dx_all.reshape(n_tok, MODEL_DIM).astype(jnp.bfloat16)
    return (out_tokens, grad_tokens, acc_up.astype(jnp.bfloat16), acc_down.astype(jnp.bfloat16))
```

```python
import functools
import math

import jax
import jax.numpy as jnp
from jax import lax
from jax.experimental import pallas as pl
from jax.experimental.pallas import tpu as pltpu
from jax.sharding import PartitionSpec as P

MESH = pl.DeviceIdType.MESH
F32 = jnp.float32
BF16 = jnp.bfloat16
NT = (((1,), (1,)), ((), ()))
OWN, RIGHT, FAR, LEFT = 0, 1, 2, 3
COLS = 512


def gelu_pair(pre_act):
    normal_cdf = 0.5 * (1.0 + lax.erf(pre_act * (2.0 ** -0.5)))
    normal_pdf = jnp.exp(-0.5 * pre_act * pre_act) * ((2.0 * math.pi) ** -0.5)
    return pre_act * normal_cdf, normal_cdf + pre_act * normal_pdf


def exchange_kernel(x_ref, dy_ref, slot_ref, gate_ref, req_ref, u_hbm, v_hbm,
                    nearp_out, nearm_out, own_out, xall_out, dyall_out, wc_out, rows_out,
                    u_v, v_v, ureq, vreq, onehot, xa, da, gall, qall, gmix, gloc, part, sib, far,
                    load_sem, out_sem, q_send, q_recv, g_send, g_recv, ax_send, ax_recv, d2d_send, d2d_recv,
                    p_send, p_recv, f_send, f_recv):
    n_dev = req_ref.shape[0]
    n_req = req_ref.shape[1]
    n_chip = n_dev // 2
    n_tok, width = x_ref.shape
    n_rows = u_v.shape[0]
    me = lax.axis_index('ep')
    core = lax.rem(me, 2)
    chip = me // 2
    other = 1 - core

    shift = n_req.bit_length() - 1

    def dev(rel, which):
        return lax.rem(chip + rel, n_chip) * 2 + which

    right, left, mate = dev(RIGHT, core), dev(LEFT, core), dev(OWN, other)
    peers = [(rel, flip) for rel in range(4) for flip in range(2) if (rel, flip) != (0, 0)]

    def peer_core(flip):
        return core if flip == 0 else other

    barrier = pltpu.get_barrier_semaphore()
    for rel, flip in peers:
        pl.semaphore_signal(barrier, inc=1, device_id={'ep': dev(rel, peer_core(flip))}, device_id_type=MESH)
    pl.semaphore_wait(barrier, len(peers))

    def rcopy(src, dst, s_sem, r_sem, target):
        return pltpu.make_async_remote_copy(src_ref=src, dst_ref=dst, send_sem=s_sem, recv_sem=r_sem, device_id={'ep': target}, device_id_type=MESH)

    load_u = pltpu.make_async_copy(u_hbm, u_v, load_sem.at[0])
    load_v = pltpu.make_async_copy(v_hbm, v_v, load_sem.at[1])

    q_copies = {}
    for n, (rel, flip) in enumerate(peers):
        back = (4 - rel) % 4
        q_copies[rel, flip] = rcopy(req_ref, qall.at[back, core], q_send.at[n], q_recv.at[n], dev(rel, peer_core(flip)))
        q_copies[rel, flip].start()
    x_right = rcopy(x_ref, xa.at[LEFT, core], ax_send.at[0], ax_recv.at[0], right)
    d_left = rcopy(dy_ref, da.at[RIGHT, core], ax_send.at[1], ax_recv.at[1], left)
    d_right = rcopy(dy_ref, da.at[LEFT, core], ax_send.at[2], ax_recv.at[2], right)
    x_left = rcopy(x_ref, xa.at[RIGHT, core], ax_send.at[3], ax_recv.at[3], left)
    x_far = rcopy(xa.at[LEFT, core], xa.at[FAR, core], ax_send.at[4], ax_recv.at[4], right)
    d_far = rcopy(da.at[RIGHT, core], da.at[FAR, core], ax_send.at[5], ax_recv.at[5], left)
    x_right.start()
    d_left.start()
    load_u.start()
    load_v.start()
    x_mate = [rcopy(x_ref if rel == OWN else xa.at[rel, core], xa.at[rel, core], d2d_send.at[rel, 0], d2d_recv.at[rel, 0], mate) for rel in range(4)]
    d_mate = [rcopy(dy_ref if rel == OWN else da.at[rel, core], da.at[rel, core], d2d_send.at[rel, 1], d2d_recv.at[rel, 1], mate) for rel in range(4)]
    x_mate[OWN].start()
    d_mate[OWN].start()
    xa[OWN, core] = x_ref[...]
    da[OWN, core] = dy_ref[...]

    own_iota = lax.broadcasted_iota(jnp.int32, (n_dev, n_req), 0)
    sub_iota = lax.broadcasted_iota(jnp.int32, (n_req, n_req), 0)

    def gate_step(step, carry):
        base = pl.multiple_of(step * 8, 8)
        s_blk = slot_ref[pl.ds(base, 8), :]
        g_blk = gate_ref[pl.ds(base, 8), :]
        for j in range(8):
            s_row = s_blk[j:j + 1, :]
            g_row = g_blk[j:j + 1, :]
            spread = jnp.where(own_iota == (s_row >> shift), g_row, 0.0)
            hi = spread.astype(BF16).astype(F32)
            rest = spread - hi
            mid = rest.astype(BF16).astype(F32)
            lo = rest - mid
            lhs = jnp.concatenate([hi, mid, lo], axis=0).astype(BF16)
            hot = jnp.where(sub_iota == (s_row & (n_req - 1)), 1.0, 0.0).astype(BF16)
            res = lax.dot_general(lhs, hot, NT, preferred_element_type=F32)
            start = pl.multiple_of((base + j) * n_dev, n_dev)
            gmix[pl.ds(start, n_dev), :] = res[0:n_dev] + res[n_dev:2 * n_dev] + res[2 * n_dev:3 * n_dev]
        return carry

    lax.fori_loop(0, n_tok // 8, gate_step, 0)
    for o in range(n_dev):
        gloc[o] = gmix[pl.ds(o, n_tok, stride=n_dev), :]

    x_right.wait_recv()
    x_far.start()
    d_left.wait_recv()
    d_far.start()
    g_copies = {}
    for n, (rel, flip) in enumerate(peers):
        back = (4 - rel) % 4
        target = dev(rel, peer_core(flip))
        g_copies[rel, flip] = rcopy(gloc.at[target], gall.at[back, core], g_send.at[n], g_recv.at[n], target)
        g_copies[rel, flip].start()
    gall[OWN, core] = gloc[me]
    d_right.start()
    x_left.start()
    x_mate[LEFT].start()
    d_mate[RIGHT].start()

    for rel, flip in peers:
        q_copies[rel, flip].wait_recv()
    qall[OWN, core] = req_ref[...]
    row_list = [qall[rel, which, pl.ds(me, 1), :] for rel in range(4) for which in range(2)]
    rows_mat = jnp.concatenate(row_list, axis=0)
    rows_out[...] = rows_mat
    rows_col = jnp.transpose(jnp.concatenate([rows_mat.astype(F32)] * (n_req // n_dev), axis=0))
    load_u.wait()
    load_v.wait()
    lane_iota = lax.broadcasted_iota(jnp.int32, (n_req, n_req), 1).astype(F32)

    def gather(rel):
        for which in range(2):
            col = jnp.broadcast_to(rows_col[:, rel * 2 + which:rel * 2 + which + 1], (n_req, n_req))
            for blk in range(n_rows // n_req):
                onehot[pl.ds(which * n_req, n_req), pl.ds(blk * n_req, n_req)] = jnp.where(col - blk * n_req == lane_iota, 1.0, 0.0).astype(BF16)

        def body(step, carry):
            cols = pl.ds(pl.multiple_of(step * COLS, COLS), COLS)
            ureq[rel, :, cols] = jnp.dot(onehot[...], u_v[:, cols], preferred_element_type=F32).astype(BF16)
            vreq[rel, :, cols] = jnp.dot(onehot[...], v_v[:, cols], preferred_element_type=F32).astype(BF16)
            return carry

        lax.fori_loop(0, width // COLS, body, 0)

    zeros = jnp.zeros((n_tok, n_req), BF16)

    def chunk(rel):
        x_blk = xa[rel].reshape(2 * n_tok, width)
        pre = lax.dot_general(x_blk, ureq[rel], NT, preferred_element_type=F32)
        dy_blk = da[rel].reshape(2 * n_tok, width)
        back_dot = lax.dot_general(dy_blk, vreq[rel], NT, preferred_element_type=F32)
        for which in range(2):
            t_lo, s_lo = which * n_tok, which * n_req
            act, slope = gelu_pair(pre[t_lo:t_lo + n_tok, s_lo:s_lo + n_req])
            gate = gall[rel, which]
            w_blk = (gate * act).astype(BF16)
            c_blk = (gate * slope * back_dot[t_lo:t_lo + n_tok, s_lo:s_lo + n_req]).astype(BF16)
            z_lo = (1 - which) * n_req
            wc_out[rel, pl.ds(t_lo, n_tok), pl.ds(s_lo, n_req)] = w_blk
            wc_out[rel, pl.ds(t_lo, n_tok), pl.ds(z_lo, n_req)] = zeros
            wc_out[rel, pl.ds(2 * n_tok + t_lo, n_tok), pl.ds(s_lo, n_req)] = c_blk
            wc_out[rel, pl.ds(2 * n_tok + t_lo, n_tok), pl.ds(z_lo, n_req)] = zeros

        def body(step, carry):
            cols = pl.ds(pl.multiple_of(step * COLS, COLS), COLS)
            part[rel, 0, :, cols] = jnp.dot(wc_out[rel, 0:2 * n_tok, :], vreq[rel, :, cols], preferred_element_type=F32)
            part[rel, 1, :, cols] = jnp.dot(wc_out[rel, 2 * n_tok:4 * n_tok, :], ureq[rel, :, cols], preferred_element_type=F32)
            return carry

        lax.fori_loop(0, width // COLS, body, 0)
        theirs = pl.ds(pl.multiple_of(other * n_tok, n_tok), n_tok)
        send = rcopy(part.at[rel, :, theirs, :], sib.at[rel], p_send.at[rel], p_recv.at[rel], mate)
        send.start()
        return send

    mine = pl.ds(pl.multiple_of(core * n_tok, n_tok), n_tok)

    def need(rel):
        for flip in range(2):
            if (rel, flip) != (0, 0):
                g_copies[(4 - rel) % 4, flip].wait_recv()
        x_mate[rel].wait_recv()
        d_mate[rel].wait_recv()

    def add_mate(rel, send):
        send.wait_recv()
        sib[rel] = sib[rel] + part[rel, :, mine, :]

    gather(FAR)
    gather(RIGHT)
    x_far.wait_recv()
    x_mate[FAR].start()
    d_far.wait_recv()
    d_mate[FAR].start()
    need(FAR)
    s_far = chunk(FAR)
    gather(LEFT)
    d_right.wait_recv()
    d_mate[LEFT].start()
    x_left.wait_recv()
    x_mate[RIGHT].start()
    add_mate(FAR, s_far)
    f_y = rcopy(sib.at[FAR, 0], far.at[0], f_send.at[0], f_recv.at[0], right)
    f_d = rcopy(sib.at[FAR, 1], far.at[1], f_send.at[1], f_recv.at[1], left)
    f_y.start()
    f_d.start()
    need(RIGHT)
    s_right = chunk(RIGHT)
    need(LEFT)
    s_left = chunk(LEFT)
    gather(OWN)
    need(OWN)
    s_own = chunk(OWN)
    o_x = pltpu.make_async_copy(xa, xall_out, out_sem.at[0])
    o_d = pltpu.make_async_copy(da, dyall_out, out_sem.at[1])
    o_x.start()
    o_d.start()
    add_mate(RIGHT, s_right)
    add_mate(LEFT, s_left)
    add_mate(OWN, s_own)
    o_own = pltpu.make_async_copy(sib.at[OWN], own_out, out_sem.at[2])
    o_own.start()
    f_y.wait_recv()
    sib[RIGHT, 0] = sib[RIGHT, 0] + far[0]
    o_right = pltpu.make_async_copy(sib.at[RIGHT], nearp_out, out_sem.at[3])
    o_right.start()
    f_d.wait_recv()
    sib[LEFT, 1] = sib[LEFT, 1] + far[1]
    o_left = pltpu.make_async_copy(sib.at[LEFT], nearm_out, out_sem.at[4])
    o_left.start()
    for key in q_copies:
        q_copies[key].wait_send()
        g_copies[key].wait_send()
    for copy in (x_right, d_left, d_right, x_left, x_far, d_far, *x_mate, *d_mate, s_far, s_right, s_left, s_own, f_y, f_d):
        copy.wait_send()
    for copy in (o_x, o_d, o_own, o_right, o_left):
        copy.wait()


def grad_kernel(rows_ref, wc_ref, xall_ref, dyall_ref, gu_ref, gv_ref, ct, wt):
    blk, width = gu_ref.shape
    n_rel = wc_ref.shape[0]
    n_tok2 = wc_ref.shape[1] // 2
    base = pl.program_id(0) * blk
    for rel in range(n_rel):
        rows = jnp.concatenate([rows_ref[2 * rel:2 * rel + 1, :], rows_ref[2 * rel + 1:2 * rel + 2, :]], axis=1)
        place = jnp.where(lax.broadcasted_iota(jnp.int32, (blk, rows.shape[1]), 0) + base == rows, 1.0, 0.0).astype(BF16)
        coef = lax.dot_general(place, wc_ref[rel], NT, preferred_element_type=F32).astype(BF16)
        wt[:, rel * n_tok2:(rel + 1) * n_tok2] = coef[:, :n_tok2]
        ct[:, rel * n_tok2:(rel + 1) * n_tok2] = coef[:, n_tok2:]
    for step in range(width // COLS):
        cols = pl.ds(step * COLS, COLS)
        gu_ref[:, cols] = jnp.dot(ct[...], xall_ref[:, cols], preferred_element_type=F32).astype(BF16)
        gv_ref[:, cols] = jnp.dot(wt[...], dyall_ref[:, cols], preferred_element_type=F32).astype(BF16)


def solution(mesh):
    n_dev = mesh.shape['ep']
    tok_spec = P(('dp', 'ep'))
    table_spec = P('ep')
    vmem = pl.BlockSpec(memory_space=pltpu.VMEM)
    hbm = pl.BlockSpec(memory_space=pl.ANY)
    dma = pltpu.SemaphoreType.DMA
    sds = jax.ShapeDtypeStruct

    def per_device(tokens, slot_ids, request_rows, gate_vals, grad_out, up_local, down_local):
        n_tok, width = tokens.shape
        n_rows = up_local.shape[0]
        n_req = request_rows.shape[2]
        sel = slot_ids.shape[1] * slot_ids.shape[2]
        n_all = n_dev * n_tok
        nearp, nearm, own, xall, dyall, wc, rows = pl.pallas_call(
            exchange_kernel,
            name='exchange',
            out_shape=(sds((2, n_tok, width), F32),) * 3 + (sds((4, 2, n_tok, width), BF16),) * 2 + (sds((4, 4 * n_tok, 2 * n_req), BF16), sds((n_dev, n_req), jnp.int32)),
            in_specs=[vmem] * 5 + [hbm] * 2,
            out_specs=(hbm,) * 5 + (vmem,) * 2,
            scratch_shapes=[
                pltpu.VMEM((n_rows, width), BF16), pltpu.VMEM((n_rows, width), BF16),
                pltpu.VMEM((4, 2 * n_req, width), BF16), pltpu.VMEM((4, 2 * n_req, width), BF16),
                pltpu.VMEM((2 * n_req, n_rows), BF16),
                pltpu.VMEM((4, 2, n_tok, width), BF16), pltpu.VMEM((4, 2, n_tok, width), BF16),
                pltpu.VMEM((4, 2, n_tok, n_req), F32), pltpu.VMEM((4, 2, n_dev, n_req), jnp.int32),
                pltpu.VMEM((n_tok * n_dev, n_req), F32), pltpu.VMEM((n_dev, n_tok, n_req), F32),
                pltpu.VMEM((4, 2, 2 * n_tok, width), F32), pltpu.VMEM((4, 2, n_tok, width), F32), pltpu.VMEM((2, n_tok, width), F32),
                dma((2,)), dma((5,)), dma((7,)), dma((7,)), dma((7,)), dma((7,)), dma((6,)), dma((6,)), dma((4, 2)), dma((4, 2)),
                dma((4,)), dma((4,)), dma((2,)), dma((2,)),
            ],
            compiler_params=pltpu.CompilerParams(collective_id=0, has_side_effects=True, vmem_limit_bytes=60 * 2 ** 20),
            cost_estimate=pl.CostEstimate(flops=4 * n_dev * n_req * n_rows * width, bytes_accessed=6 * n_rows * width, transcendentals=0),
        )(tokens, grad_out, slot_ids.reshape(n_tok, sel), gate_vals.reshape(n_tok, sel), request_rows[0], up_local, down_local)

        up_chip = [(d, (d + 2) % n_dev) for d in range(n_dev)]
        down_chip = [(d, (d - 2) % n_dev) for d in range(n_dev)]
        from_left = lax.ppermute(nearp, 'ep', up_chip)
        from_right = lax.ppermute(nearm, 'ep', down_chip)

        blk = min(256, n_rows)
        full = lambda shape: pl.BlockSpec(shape, lambda i: (0,) * len(shape))
        grad_up, grad_down = pl.pallas_call(
            grad_kernel,
            name='table_grads',
            out_shape=(sds((n_rows, width), BF16),) * 2,
            grid=(n_rows // blk,),
            in_specs=[full(rows.shape), full(wc.shape), full((n_all, width)), full((n_all, width))],
            out_specs=(pl.BlockSpec((blk, width), lambda i: (i, 0)),) * 2,
            scratch_shapes=[pltpu.VMEM((blk, n_all), BF16)] * 2,
            compiler_params=pltpu.CompilerParams(vmem_limit_bytes=40 * 2 ** 20),
            cost_estimate=pl.CostEstimate(flops=4 * n_rows * n_all * width, bytes_accessed=4 * (n_rows + n_all) * width, transcendentals=0),
        )(rows, wc, xall.reshape(n_all, width), dyall.reshape(n_all, width))
        total = (own + from_left + from_right).astype(BF16)
        return total[0], total[1], grad_up, grad_down

    return jax.shard_map(per_device, mesh=mesh, in_specs=(tok_spec, tok_spec, tok_spec, tok_spec, tok_spec, table_spec, table_spec), out_specs=(tok_spec, tok_spec, tok_spec, tok_spec), check_vma=False)
```

```python
import functools
import math

import jax
import jax.numpy as jnp
from jax import lax
from jax.experimental import pallas as pl
from jax.experimental.pallas import tpu as pltpu
from jax.sharding import PartitionSpec as P

MESH = pl.DeviceIdType.MESH
F32 = jnp.float32
BF16 = jnp.bfloat16
NT = (((1,), (1,)), ((), ()))
OWN, RIGHT, FAR, LEFT = 0, 1, 2, 3
ORDER = (RIGHT, LEFT, FAR, OWN)
COLS = 512
WIDE = 1024
LATE = 256


def gelu_pair(pre_act):
    normal_cdf = 0.5 * (1.0 + lax.erf(pre_act * (2.0 ** -0.5)))
    normal_pdf = jnp.exp(-0.5 * pre_act * pre_act) * ((2.0 * math.pi) ** -0.5)
    return pre_act * normal_cdf, normal_cdf + pre_act * normal_pdf


def exchange_kernel(x_hbm, dy_hbm, slot_hbm, gate_hbm, req_hbm, u_hbm, v_hbm,
                    y_next, dx_next, own_out, xall_out, dyall_out, ct_out, wt_out,
                    u_v, v_v, ureq, vreq, onehot, xa, da, gall, qall, slot_in, gate_in, slots, gates, gmix, gloc, wc, ct, wt, part, sib, near, far,
                    load_sem, out_sem, q_send, q_recv, g_send, g_recv, ax_send, ax_recv, d2d_send, d2d_recv,
                    p_send, p_recv, n_send, n_recv, f_send, f_recv):
    n_dev, n_req = req_hbm.shape
    n_chip = n_dev // 2
    n_tok, width = x_hbm.shape
    n_rows = u_v.shape[0]
    shift = n_req.bit_length() - 1
    me = lax.axis_index('ep')
    core = lax.rem(me, 2)
    chip = me // 2
    other = 1 - core

    def dev(rel, which):
        return lax.rem(chip + rel, n_chip) * 2 + which

    right, left, mate = dev(RIGHT, core), dev(LEFT, core), dev(OWN, other)
    peers = [(rel, flip) for rel in range(4) for flip in range(2) if (rel, flip) != (0, 0)]

    def peer_core(flip):
        return core if flip == 0 else other

    barrier = pltpu.get_barrier_semaphore()
    for rel, flip in peers:
        pl.semaphore_signal(barrier, inc=1, device_id={'ep': dev(rel, peer_core(flip))}, device_id_type=MESH)

    load_x = pltpu.make_async_copy(x_hbm, xa.at[OWN, core], load_sem.at[0])
    load_d = pltpu.make_async_copy(dy_hbm, da.at[OWN, core], load_sem.at[1])
    load_q = pltpu.make_async_copy(req_hbm, qall.at[OWN, core], load_sem.at[2])
    load_s = pltpu.make_async_copy(slot_hbm, slot_in, load_sem.at[3])
    load_g = pltpu.make_async_copy(gate_hbm, gate_in, load_sem.at[4])
    load_u = pltpu.make_async_copy(u_hbm, u_v, load_sem.at[5])
    load_v = pltpu.make_async_copy(v_hbm, v_v, load_sem.at[6])
    for load in (load_q, load_x, load_d, load_s, load_g, load_u, load_v):
        load.start()

    def rcopy(src, dst, s_sem, r_sem, target):
        return pltpu.make_async_remote_copy(src_ref=src, dst_ref=dst, send_sem=s_sem, recv_sem=r_sem, device_id={'ep': target}, device_id_type=MESH)

    q_copies, g_copies = {}, {}
    for n, (rel, flip) in enumerate(peers):
        back = (4 - rel) % 4
        target = dev(rel, peer_core(flip))
        q_copies[rel, flip] = rcopy(qall.at[OWN, core], qall.at[back, core], q_send.at[n], q_recv.at[n], target)
        g_copies[rel, flip] = rcopy(gloc.at[target], gall.at[back, core], g_send.at[n], g_recv.at[n], target)
    x_right = rcopy(xa.at[OWN, core], xa.at[LEFT, core], ax_send.at[0], ax_recv.at[0], right)
    d_left = rcopy(da.at[OWN, core], da.at[RIGHT, core], ax_send.at[1], ax_recv.at[1], left)
    d_right = rcopy(da.at[OWN, core], da.at[LEFT, core], ax_send.at[2], ax_recv.at[2], right)
    x_left = rcopy(xa.at[OWN, core], xa.at[RIGHT, core], ax_send.at[3], ax_recv.at[3], left)
    x_far = rcopy(xa.at[LEFT, core], xa.at[FAR, core], ax_send.at[4], ax_recv.at[4], right)
    d_far = rcopy(da.at[RIGHT, core], da.at[FAR, core], ax_send.at[5], ax_recv.at[5], left)
    x_mate = [rcopy(xa.at[rel, core], xa.at[rel, core], d2d_send.at[rel, 0], d2d_recv.at[rel, 0], mate) for rel in range(4)]
    d_mate = [rcopy(da.at[rel, core], da.at[rel, core], d2d_send.at[rel, 1], d2d_recv.at[rel, 1], mate) for rel in range(4)]

    load_q.wait()
    load_x.wait()
    load_d.wait()
    pl.semaphore_wait(barrier, len(peers))
    near_peers = [key for key in peers if key[0] != FAR]
    far_peers = [key for key in peers if key[0] == FAR]
    for key in near_peers:
        q_copies[key].start()
    x_right.start()
    d_left.start()
    for key in far_peers:
        q_copies[key].start()
    d_right.start()
    x_left.start()
    x_mate[OWN].start()
    d_mate[OWN].start()
    load_s.wait()
    load_g.wait()
    slots[...] = jnp.transpose(slot_in[...].astype(F32)).astype(jnp.int32)
    gates[...] = jnp.transpose(gate_in[...])

    own_iota = lax.broadcasted_iota(jnp.int32, (n_dev, n_req), 0)
    sub_iota = lax.broadcasted_iota(jnp.int32, (n_req, n_req), 0)

    def gate_step(step, carry):
        base = pl.multiple_of(step * 8, 8)
        s_blk = slots[pl.ds(base, 8), :]
        g_blk = gates[pl.ds(base, 8), :]
        for j in range(8):
            s_row = s_blk[j:j + 1, :]
            g_row = g_blk[j:j + 1, :]
            spread = jnp.where(own_iota == (s_row >> shift), g_row, 0.0)
            hi = spread.astype(BF16).astype(F32)
            rest = spread - hi
            mid = rest.astype(BF16).astype(F32)
            lo = rest - mid
            lhs = jnp.concatenate([hi, mid, lo], axis=0).astype(BF16)
            hot = jnp.where(sub_iota == (s_row & (n_req - 1)), 1.0, 0.0).astype(BF16)
            res = lax.dot_general(lhs, hot, NT, preferred_element_type=F32)
            start = pl.multiple_of((base + j) * n_dev, n_dev)
            gmix[pl.ds(start, n_dev), :] = res[0:n_dev] + res[n_dev:2 * n_dev] + res[2 * n_dev:3 * n_dev]
        return carry

    lax.fori_loop(0, n_tok // 8, gate_step, 0)
    for o in range(n_dev):
        gloc[o] = gmix[pl.ds(o, n_tok, stride=n_dev), :]
    for key in near_peers + far_peers:
        g_copies[key].start()
    gall[OWN, core] = gloc[me]

    lane_iota = lax.broadcasted_iota(jnp.int32, (n_req, n_req), 1).astype(F32)

    def lists(rel):
        return [qall[rel, which, pl.ds(me, 1), :] for which in range(2)]

    def gather_hot(rels):
        rows = [r.astype(F32) for rel in rels for r in lists(rel)]
        stack = jnp.broadcast_to(rows[0], (n_req, n_req))
        for n in range(1, len(rows)):
            stack = jnp.where(sub_iota == n, rows[n], stack)
        cols = jnp.transpose(stack)
        for n in range(len(rows)):
            col = jnp.broadcast_to(cols[:, n:n + 1], (n_req, n_req))
            for blk in range(n_rows // n_req):
                onehot[pl.ds(n * n_req, n_req), pl.ds(blk * n_req, n_req)] = jnp.where(col - blk * n_req == lane_iota, 1.0, 0.0).astype(BF16)

    def gather_rows(rels, src, dst, first, last):
        size = len(rels) * 2 * n_req
        base = ORDER.index(rels[0]) * 2 * n_req

        def body(step, carry):
            cols = pl.ds(pl.multiple_of(step * WIDE, WIDE), WIDE)
            dst[base:base + size, cols] = jnp.dot(onehot[0:size, :], src[:, cols], preferred_element_type=F32).astype(BF16)
            return carry

        lax.fori_loop(first, last, body, 0)

    def rows_of(table, rel, cols=slice(None)):
        base = ORDER.index(rel) * 2 * n_req
        return table[base:base + 2 * n_req, cols]

    zeros = jnp.zeros((n_tok, n_req), BF16)

    def scores(rel):
        pre = lax.dot_general(xa[rel].reshape(2 * n_tok, width), rows_of(ureq, rel), NT, preferred_element_type=F32)
        back_dot = lax.dot_general(da[rel].reshape(2 * n_tok, width), rows_of(vreq, rel), NT, preferred_element_type=F32)
        for flip in range(2):
            if (rel, flip) != (0, 0):
                g_copies[(4 - rel) % 4, flip].wait_recv()
        for which in range(2):
            t_lo, s_lo = which * n_tok, which * n_req
            act, slope = gelu_pair(pre[t_lo:t_lo + n_tok, s_lo:s_lo + n_req])
            gate = gall[rel, which]
            z_lo = (1 - which) * n_req
            wc[rel, pl.ds(t_lo, n_tok), pl.ds(s_lo, n_req)] = (gate * act).astype(BF16)
            wc[rel, pl.ds(t_lo, n_tok), pl.ds(z_lo, n_req)] = zeros
            wc[rel, pl.ds(2 * n_tok + t_lo, n_tok), pl.ds(s_lo, n_req)] = (gate * slope * back_dot[t_lo:t_lo + n_tok, s_lo:s_lo + n_req]).astype(BF16)
            wc[rel, pl.ds(2 * n_tok + t_lo, n_tok), pl.ds(z_lo, n_req)] = zeros

    theirs = pl.ds(pl.multiple_of(other * n_tok, n_tok), n_tok)
    mine = pl.ds(pl.multiple_of(core * n_tok, n_tok), n_tok)

    def partial(rel, out):
        table = vreq if out == 0 else ureq

        def body(step, carry):
            cols = pl.ds(pl.multiple_of(step * COLS, COLS), COLS)
            part[rel, out, :, cols] = jnp.dot(wc[rel, out * 2 * n_tok:(out + 1) * 2 * n_tok, :], rows_of(table, rel, cols), preferred_element_type=F32)
            return carry

        lax.fori_loop(0, width // COLS, body, 0)
        send = rcopy(part.at[rel, out, theirs, :], sib.at[rel, out], p_send.at[rel, out], p_recv.at[rel, out], mate)
        send.start()
        return send

    def add_mate(rel, out, send):
        send.wait_recv()
        sib[rel, out] = sib[rel, out] + part[rel, out, mine, :]

    def place(rel):
        rows = jnp.concatenate(lists(rel), axis=1)
        blk = n_rows // 2

        def body(step, carry):
            base = pl.multiple_of(step * blk, blk)
            hot = jnp.where(lax.broadcasted_iota(jnp.int32, (blk, 2 * n_req), 0) + base == rows, 1.0, 0.0).astype(BF16)
            coef = lax.dot_general(hot, wc[rel], NT, preferred_element_type=F32).astype(BF16)
            wt[pl.ds(base, blk), rel * 2 * n_tok:(rel + 1) * 2 * n_tok] = coef[:, :2 * n_tok]
            ct[pl.ds(base, blk), rel * 2 * n_tok:(rel + 1) * 2 * n_tok] = coef[:, 2 * n_tok:]
            return carry

        lax.fori_loop(0, n_rows // blk, body, 0)

    def need(rel):
        x_mate[rel].wait_recv()
        d_mate[rel].wait_recv()

    n_wide = width // WIDE
    cut = width - LATE
    for rel, flip in near_peers:
        q_copies[rel, flip].wait_recv()
    gather_hot((RIGHT, LEFT))
    load_u.wait()
    gather_rows((RIGHT, LEFT), u_v, ureq, 0, n_wide)
    x_right.wait_recv()
    x_far.start()
    x_mate[LEFT].start()
    d_left.wait_recv()
    d_far.start()
    d_mate[RIGHT].start()
    load_v.wait()
    gather_rows((RIGHT, LEFT), v_v, vreq, 0, n_wide)
    for rel, flip in far_peers:
        q_copies[rel, flip].wait_recv()
    gather_hot((FAR,))
    gather_rows((FAR,), u_v, ureq, 0, 1)
    d_right.wait_recv()
    d_mate[LEFT].start()
    x_left.wait_recv()
    x_mate[RIGHT].start()
    gather_rows((FAR,), u_v, ureq, 1, n_wide)
    need(RIGHT)
    scores(RIGHT)
    s_right_d = partial(RIGHT, 1)
    need(LEFT)
    scores(LEFT)
    s_left_y = partial(LEFT, 0)
    add_mate(RIGHT, 1, s_right_d)
    n_right = rcopy(sib.at[RIGHT, 1, :, 0:cut], near.at[1], n_send.at[1], n_recv.at[1], right)
    n_right.start()
    add_mate(LEFT, 0, s_left_y)
    n_left = rcopy(sib.at[LEFT, 0, :, 0:cut], near.at[0], n_send.at[0], n_recv.at[0], left)
    n_left.start()
    gather_rows((FAR,), v_v, vreq, 0, n_wide)
    x_far.wait_recv()
    x_mate[FAR].start()
    d_far.wait_recv()
    d_mate[FAR].start()
    s_right_y = partial(RIGHT, 0)
    s_left_d = partial(LEFT, 1)
    need(FAR)
    scores(FAR)
    s_far = [partial(FAR, 0), partial(FAR, 1)]
    add_mate(FAR, 0, s_far[0])
    f_y = rcopy(sib.at[FAR, 0], far.at[0], f_send.at[0], f_recv.at[0], right)
    f_y.start()
    add_mate(FAR, 1, s_far[1])
    f_d = rcopy(sib.at[FAR, 1], far.at[1], f_send.at[1], f_recv.at[1], left)
    f_d.start()
    gather_hot((OWN,))
    gather_rows((OWN,), u_v, ureq, 0, n_wide)
    gather_rows((OWN,), v_v, vreq, 0, n_wide)
    need(OWN)
    scores(OWN)
    s_own = [partial(OWN, 0), partial(OWN, 1)]
    o_x = pltpu.make_async_copy(xa, xall_out, out_sem.at[0])
    o_d = pltpu.make_async_copy(da, dyall_out, out_sem.at[1])
    o_x.start()
    o_d.start()
    for rel in range(4):
        place(rel)
    o_c = pltpu.make_async_copy(ct, ct_out, out_sem.at[2])
    o_w = pltpu.make_async_copy(wt, wt_out, out_sem.at[3])
    o_c.start()
    o_w.start()
    add_mate(RIGHT, 0, s_right_y)
    add_mate(LEFT, 1, s_left_d)
    add_mate(OWN, 0, s_own[0])
    add_mate(OWN, 1, s_own[1])
    n_left.wait_recv()
    sib[OWN, 0, :, 0:cut] = sib[OWN, 0, :, 0:cut] + near[0]
    n_right.wait_recv()
    sib[OWN, 1, :, 0:cut] = sib[OWN, 1, :, 0:cut] + near[1]
    o_own = pltpu.make_async_copy(sib.at[OWN], own_out, out_sem.at[4])
    o_own.start()
    o_rest = [pltpu.make_async_copy(sib.at[RIGHT, 1, :, cut:width], y_next.at[:, width:width + LATE], out_sem.at[7]),
              pltpu.make_async_copy(sib.at[LEFT, 0, :, cut:width], dx_next.at[:, width:width + LATE], out_sem.at[8])]
    for copy in o_rest:
        copy.start()
    for key in q_copies:
        q_copies[key].wait_send()
        g_copies[key].wait_send()
    for copy in (x_right, d_left, d_right, x_left, x_far, d_far, *x_mate, *d_mate, *s_far, s_right_d, s_right_y, s_left_y, s_left_d, *s_own, n_left, n_right):
        copy.wait_send()
    for copy in (o_x, o_d, o_c, o_w, o_own, *o_rest):
        copy.wait()
    f_y.wait_recv()
    sib[RIGHT, 0] = sib[RIGHT, 0] + far[0]
    o_y = pltpu.make_async_copy(sib.at[RIGHT, 0], y_next.at[:, 0:width], out_sem.at[5])
    o_y.start()
    f_d.wait_recv()
    sib[LEFT, 1] = sib[LEFT, 1] + far[1]
    o_dx = pltpu.make_async_copy(sib.at[LEFT, 1], dx_next.at[:, 0:width], out_sem.at[6])
    o_dx.start()
    f_y.wait_send()
    f_d.wait_send()
    o_y.wait()
    o_dx.wait()


def grad_kernel(ct_ref, wt_ref, xall_ref, dyall_ref, gu_ref, gv_ref):
    width = gu_ref.shape[1]
    for step in range(width // WIDE):
        cols = pl.ds(step * WIDE, WIDE)
        gu_ref[:, cols] = jnp.dot(ct_ref[...], xall_ref[:, cols], preferred_element_type=F32).astype(BF16)
        gv_ref[:, cols] = jnp.dot(wt_ref[...], dyall_ref[:, cols], preferred_element_type=F32).astype(BF16)


def solution(mesh):
    n_dev = mesh.shape['ep']
    tok_spec = P(('dp', 'ep'))
    table_spec = P('ep')
    hbm = pl.BlockSpec(memory_space=pl.ANY)
    dma = pltpu.SemaphoreType.DMA
    sds = jax.ShapeDtypeStruct

    def per_device(tokens, slot_ids, request_rows, gate_vals, grad_out, up_local, down_local):
        n_tok, width = tokens.shape
        n_rows = up_local.shape[0]
        n_req = request_rows.shape[2]
        sel = slot_ids.shape[1] * slot_ids.shape[2]
        n_all = n_dev * n_tok
        y_next, dx_next, own, xall, dyall, ct, wt = pl.pallas_call(
            exchange_kernel,
            name='exchange',
            out_shape=(sds((n_tok, width + LATE), F32), sds((n_tok, width + LATE), F32), sds((2, n_tok, width), F32),
                       sds((4, 2, n_tok, width), BF16), sds((4, 2, n_tok, width), BF16), sds((n_rows, n_all), BF16), sds((n_rows, n_all), BF16)),
            in_specs=[hbm] * 7,
            out_specs=(hbm,) * 7,
            scratch_shapes=[
                pltpu.VMEM((n_rows, width), BF16), pltpu.VMEM((n_rows, width), BF16),
                pltpu.VMEM((n_dev * n_req, width), BF16), pltpu.VMEM((n_dev * n_req, width), BF16),
                pltpu.VMEM((4 * n_req, n_rows), BF16),
                pltpu.VMEM((4, 2, n_tok, width), BF16), pltpu.VMEM((4, 2, n_tok, width), BF16),
                pltpu.VMEM((4, 2, n_tok, n_req), F32), pltpu.VMEM((4, 2, n_dev, n_req), jnp.int32),
                pltpu.VMEM((sel, n_tok), jnp.int32), pltpu.VMEM((sel, n_tok), F32), pltpu.VMEM((n_tok, sel), jnp.int32), pltpu.VMEM((n_tok, sel), F32),
                pltpu.VMEM((n_tok * n_dev, n_req), F32), pltpu.VMEM((n_dev, n_tok, n_req), F32),
                pltpu.VMEM((4, 4 * n_tok, 2 * n_req), BF16), pltpu.VMEM((n_rows, n_all), BF16), pltpu.VMEM((n_rows, n_all), BF16),
                pltpu.VMEM((4, 2, 2 * n_tok, width), F32), pltpu.VMEM((4, 2, n_tok, width), F32),
                pltpu.VMEM((2, n_tok, width - LATE), F32), pltpu.VMEM((2, n_tok, width), F32),
                dma((7,)), dma((9,)), dma((7,)), dma((7,)), dma((7,)), dma((7,)), dma((6,)), dma((6,)), dma((4, 2)), dma((4, 2)),
                dma((4, 2)), dma((4, 2)), dma((2,)), dma((2,)), dma((2,)), dma((2,)),
            ],
            compiler_params=pltpu.CompilerParams(collective_id=0, has_side_effects=True, vmem_limit_bytes=60 * 2 ** 20),
            cost_estimate=pl.CostEstimate(flops=4 * n_dev * n_req * n_rows * width, bytes_accessed=6 * n_rows * width, transcendentals=0),
        )(tokens, grad_out, slot_ids.reshape(n_tok, sel).T, gate_vals.reshape(n_tok, sel).T, request_rows[0], up_local, down_local)

        up_chip = [(d, (d + 2) % n_dev) for d in range(n_dev)]
        down_chip = [(d, (d - 2) % n_dev) for d in range(n_dev)]
        y_last = lax.ppermute(y_next, 'ep', up_chip)
        dx_last = lax.ppermute(dx_next, 'ep', down_chip)

        blk = min(512, n_rows)
        row_spec = lambda cols: pl.BlockSpec((blk, cols), lambda i: (i, 0))
        full_spec = pl.BlockSpec((n_all, width), lambda i: (0, 0))
        grad_up, grad_down = pl.pallas_call(
            grad_kernel,
            name='table_grads',
            out_shape=(sds((n_rows, width), BF16),) * 2,
            grid=(n_rows // blk,),
            in_specs=[row_spec(n_all), row_spec(n_all), full_spec, full_spec],
            out_specs=(row_spec(width),) * 2,
            compiler_params=pltpu.CompilerParams(vmem_limit_bytes=60 * 2 ** 20),
            cost_estimate=pl.CostEstimate(flops=4 * n_rows * n_all * width, bytes_accessed=4 * (n_rows + n_all) * width, transcendentals=0),
        )(ct, wt, xall.reshape(n_all, width), dyall.reshape(n_all, width))
        rest = lambda a: jnp.pad(a[:, width:], ((0, 0), (width - LATE, 0)))
        y = own[0] + y_last[:, :width] + rest(dx_last)
        dx = own[1] + dx_last[:, :width] + rest(y_last)
        return y.astype(BF16), dx.astype(BF16), grad_up, grad_down

    return jax.shard_map(per_device, mesh=mesh, in_specs=(tok_spec, tok_spec, tok_spec, tok_spec, tok_spec, table_spec, table_spec), out_specs=(tok_spec, tok_spec, tok_spec, tok_spec), check_vma=False)
```

```python
import functools
import math

import jax
import jax.numpy as jnp
from jax import lax
from jax.experimental import pallas as pl
from jax.experimental.pallas import tpu as pltpu
from jax.sharding import PartitionSpec as P

MESH = pl.DeviceIdType.MESH
F32 = jnp.float32
BF16 = jnp.bfloat16
NT = (((1,), (1,)), ((), ()))
OWN, RIGHT, FAR, LEFT = 0, 1, 2, 3
ORDER = (RIGHT, LEFT, FAR, OWN)
COLS = 512
WIDE = 1024
LATE = 512
HALVES = 2


def gelu_pair(pre_act):
    normal_cdf = 0.5 * (1.0 + lax.erf(pre_act * (2.0 ** -0.5)))
    normal_pdf = jnp.exp(-0.5 * pre_act * pre_act) * ((2.0 * math.pi) ** -0.5)
    return pre_act * normal_cdf, normal_cdf + pre_act * normal_pdf


def exchange_kernel(x_hbm, dy_hbm, slot_hbm, gate_hbm, req_hbm, u_hbm, v_hbm,
                    y_next, dx_next, own_out, xall_out, dyall_out, ct_out, wt_out,
                    u_v, v_v, ureq, vreq, onehot, xa, da, gall, qall, gpass, slot_in, gate_in, slots, gates, gmix, gloc, dots_x, dots_d, wc, ct, wt, part, sib, near, far,
                    load_sem, out_sem, q_send, q_recv, g_send, g_recv, ax_send, ax_recv, d2d_send, d2d_recv,
                    p_send, p_recv, n_send, n_recv, f_send, f_recv):
    n_dev, n_req = req_hbm.shape
    n_chip = n_dev // 2
    n_tok, width = x_hbm.shape
    n_rows = u_v.shape[0]
    shift = n_req.bit_length() - 1
    me = lax.axis_index('ep')
    core = lax.rem(me, 2)
    chip = me // 2
    other = 1 - core

    def dev(rel, which):
        return lax.rem(chip + rel, n_chip) * 2 + which

    right, left, mate = dev(RIGHT, core), dev(LEFT, core), dev(OWN, other)
    peers = [(rel, flip) for rel in (OWN, RIGHT, LEFT) for flip in range(2) if (rel, flip) != (OWN, 0)]

    def peer_core(flip):
        return core if flip == 0 else other

    barrier = pltpu.get_barrier_semaphore()
    for rel, flip in peers:
        pl.semaphore_signal(barrier, inc=1, device_id={'ep': dev(rel, peer_core(flip))}, device_id_type=MESH)

    load_x = pltpu.make_async_copy(x_hbm, xa.at[OWN, core], load_sem.at[0])
    load_d = pltpu.make_async_copy(dy_hbm, da.at[OWN, core], load_sem.at[1])
    load_q = pltpu.make_async_copy(req_hbm, qall.at[OWN, core], load_sem.at[2])
    load_s = pltpu.make_async_copy(slot_hbm, slot_in, load_sem.at[3])
    load_g = pltpu.make_async_copy(gate_hbm, gate_in, load_sem.at[4])
    load_u = pltpu.make_async_copy(u_hbm, u_v, load_sem.at[5])
    load_v = pltpu.make_async_copy(v_hbm, v_v, load_sem.at[6])
    for load in (load_q, load_x, load_d, load_s, load_g, load_u, load_v):
        load.start()

    def rcopy(src, dst, s_sem, r_sem, target):
        return pltpu.make_async_remote_copy(src_ref=src, dst_ref=dst, send_sem=s_sem, recv_sem=r_sem, device_id={'ep': target}, device_id_type=MESH)

    q_copies, g_copies = {}, {}
    for n, (rel, flip) in enumerate(peers):
        back = (4 - rel) % 4
        target = dev(rel, peer_core(flip))
        q_copies[rel, flip] = rcopy(qall.at[OWN, core], qall.at[back, core], q_send.at[n], q_recv.at[n], target)
        g_copies[rel, flip] = rcopy(gloc.at[target], gall.at[back, core], g_send.at[n], g_recv.at[n], target)
    q_pass = [rcopy(qall.at[LEFT, core], qall.at[FAR, core], q_send.at[5 + flip], q_recv.at[5 + flip], dev(RIGHT, peer_core(flip))) for flip in range(2)]
    g_out = [rcopy(gloc.at[dev(FAR, peer_core(flip))], gpass.at[flip], g_send.at[5 + flip], g_recv.at[5 + flip], (right, left)[flip]) for flip in range(2)]
    g_pass = [rcopy(gpass.at[flip], gall.at[FAR, core], g_send.at[7 + flip], g_recv.at[7 + flip], dev((RIGHT, LEFT)[flip], peer_core(flip))) for flip in range(2)]
    x_right = rcopy(xa.at[OWN, core], xa.at[LEFT, core], ax_send.at[0], ax_recv.at[0], right)
    d_left = rcopy(da.at[OWN, core], da.at[RIGHT, core], ax_send.at[1], ax_recv.at[1], left)
    d_right = rcopy(da.at[OWN, core], da.at[LEFT, core], ax_send.at[2], ax_recv.at[2], right)
    x_left = rcopy(xa.at[OWN, core], xa.at[RIGHT, core], ax_send.at[3], ax_recv.at[3], left)
    x_far = rcopy(xa.at[LEFT, core], xa.at[FAR, core], ax_send.at[4], ax_recv.at[4], right)
    d_far = rcopy(da.at[RIGHT, core], da.at[FAR, core], ax_send.at[5], ax_recv.at[5], left)
    x_mate = [rcopy(xa.at[rel, core], xa.at[rel, core], d2d_send.at[rel, 0], d2d_recv.at[rel, 0], mate) for rel in range(4)]
    d_mate = [rcopy(da.at[rel, core], da.at[rel, core], d2d_send.at[rel, 1], d2d_recv.at[rel, 1], mate) for rel in range(4)]

    load_q.wait()
    load_x.wait()
    load_d.wait()
    pl.semaphore_wait(barrier, len(peers))
    for key in peers:
        q_copies[key].start()
    x_right.start()
    d_left.start()
    x_mate[OWN].start()
    d_mate[OWN].start()
    load_s.wait()
    load_g.wait()
    slots[...] = jnp.transpose(slot_in[...].astype(F32)).astype(jnp.int32)
    gates[...] = jnp.transpose(gate_in[...])

    own_iota = lax.broadcasted_iota(jnp.int32, (n_dev, n_req), 0)
    sub_iota = lax.broadcasted_iota(jnp.int32, (n_req, n_req), 0)

    def gate_step(step, carry):
        base = pl.multiple_of(step * 8, 8)
        s_blk = slots[pl.ds(base, 8), :]
        g_blk = gates[pl.ds(base, 8), :]
        for j in range(8):
            s_row = s_blk[j:j + 1, :]
            g_row = g_blk[j:j + 1, :]
            spread = jnp.where(own_iota == (s_row >> shift), g_row, 0.0)
            hi = spread.astype(BF16).astype(F32)
            rest = spread - hi
            mid = rest.astype(BF16).astype(F32)
            lo = rest - mid
            lhs = jnp.concatenate([hi, mid, lo], axis=0).astype(BF16)
            hot = jnp.where(sub_iota == (s_row & (n_req - 1)), 1.0, 0.0).astype(BF16)
            res = lax.dot_general(lhs, hot, NT, preferred_element_type=F32)
            start = pl.multiple_of((base + j) * n_dev, n_dev)
            gmix[pl.ds(start, n_dev), :] = res[0:n_dev] + res[n_dev:2 * n_dev] + res[2 * n_dev:3 * n_dev]
        return carry

    lax.fori_loop(0, n_tok // 8, gate_step, 0)
    for o in range(n_dev):
        gloc[o] = gmix[pl.ds(o, n_tok, stride=n_dev), :]
    for key in peers:
        q_copies[key].wait_recv()
    for copy in q_pass:
        copy.start()
    d_right.start()
    x_left.start()
    for copy in g_out:
        copy.start()
    for key in peers:
        g_copies[key].start()
    gall[OWN, core] = gloc[me]

    lane_iota = lax.broadcasted_iota(jnp.int32, (n_req, n_req), 1).astype(F32)

    def lists(rel):
        return [qall[rel, which, pl.ds(me, 1), :] for which in range(2)]

    def gather_hot(rels):
        rows = [r.astype(F32) for rel in rels for r in lists(rel)]
        stack = jnp.broadcast_to(rows[0], (n_req, n_req))
        for n in range(1, len(rows)):
            stack = jnp.where(sub_iota == n, rows[n], stack)
        cols = jnp.transpose(stack)
        for n in range(len(rows)):
            col = jnp.broadcast_to(cols[:, n:n + 1], (n_req, n_req))
            for blk in range(n_rows // n_req):
                onehot[pl.ds(n * n_req, n_req), pl.ds(blk * n_req, n_req)] = jnp.where(col - blk * n_req == lane_iota, 1.0, 0.0).astype(BF16)

    def gather_rows(rels, src, dst, first, last):
        size = len(rels) * 2 * n_req
        base = ORDER.index(rels[0]) * 2 * n_req

        def body(step, carry):
            cols = pl.ds(pl.multiple_of(step * WIDE, WIDE), WIDE)
            dst[base:base + size, cols] = jnp.dot(onehot[0:size, :], src[:, cols], preferred_element_type=F32).astype(BF16)
            return carry

        lax.fori_loop(first, last, body, 0)

    def rows_of(table, rel, cols=slice(None)):
        base = ORDER.index(rel) * 2 * n_req
        return table[base:base + 2 * n_req, cols]

    zeros = jnp.zeros((n_tok, n_req), BF16)

    def tokens_of(buf, rel):
        return buf[rel].reshape(2 * n_tok, width)

    def dot_x(rel):
        dots_x[rel] = lax.dot_general(tokens_of(xa, rel), rows_of(ureq, rel), NT, preferred_element_type=F32)

    def dot_d(rel):
        dots_d[rel] = lax.dot_general(tokens_of(da, rel), rows_of(vreq, rel), NT, preferred_element_type=F32)

    def gates_here(rel):
        for flip in range(2):
            if rel == FAR:
                g_pass[flip].wait_recv()
            elif (rel, flip) != (OWN, 0):
                g_copies[(4 - rel) % 4, flip].wait_recv()

    def coef(rel, out):
        for which in range(2):
            toks, slot = pl.ds(which * n_tok, n_tok), pl.ds(which * n_req, n_req)
            act, slope = gelu_pair(dots_x[rel, toks, slot])
            value = gall[rel, which] * (act if out == 0 else slope)
            if out == 1:
                value = value * dots_d[rel, toks, slot]
            row = pl.ds((out * 2 + which) * n_tok, n_tok)
            wc[rel, row, slot] = value.astype(BF16)
            wc[rel, row, pl.ds((1 - which) * n_req, n_req)] = zeros

    theirs = pl.ds(pl.multiple_of(other * n_tok, n_tok), n_tok)
    mine = pl.ds(pl.multiple_of(core * n_tok, n_tok), n_tok)

    span = [pl.ds(h * width // HALVES, width // HALVES) for h in range(HALVES)]

    def partial(rel, out):
        table = vreq if out == 0 else ureq
        sends = []
        for h, cols in enumerate(span):
            part[rel, out, :, cols] = jnp.dot(wc[rel, out * 2 * n_tok:(out + 1) * 2 * n_tok, :], rows_of(table, rel, cols), preferred_element_type=F32)
            sends.append(rcopy(part.at[rel, out, theirs, cols], sib.at[rel, out, :, cols], p_send.at[rel, out, h], p_recv.at[rel, out, h], mate))
            sends[-1].start()
        return sends

    def add_mate(rel, out, sends, h):
        sends[h].wait_recv()
        sib[rel, out, :, span[h]] = sib[rel, out, :, span[h]] + part[rel, out, mine, span[h]]

    def place(rel):
        rows = jnp.concatenate(lists(rel), axis=1)
        blk = n_rows // 2

        def body(step, carry):
            base = pl.multiple_of(step * blk, blk)
            hot = jnp.where(lax.broadcasted_iota(jnp.int32, (blk, 2 * n_req), 0) + base == rows, 1.0, 0.0).astype(BF16)
            coef = lax.dot_general(hot, wc[rel], NT, preferred_element_type=F32).astype(BF16)
            wt[pl.ds(base, blk), rel * 2 * n_tok:(rel + 1) * 2 * n_tok] = coef[:, :2 * n_tok]
            ct[pl.ds(base, blk), rel * 2 * n_tok:(rel + 1) * 2 * n_tok] = coef[:, 2 * n_tok:]
            return carry

        lax.fori_loop(0, n_rows // blk, body, 0)

    n_wide = width // WIDE
    cut = width - LATE
    part_half = width // HALVES
    early = [pl.ds(h * part_half, min(part_half, cut - h * part_half)) for h in range(HALVES)]

    def send_near(rel, out, sends, target):
        copies = []
        for h in range(HALVES):
            add_mate(rel, out, sends, h)
            copies.append(rcopy(sib.at[rel, out, :, early[h]], near.at[out, :, early[h]], n_send.at[out, h], n_recv.at[out, h], target))
            copies[-1].start()
        return copies

    def send_far(out, sends, target):
        copies = []
        for h in range(HALVES):
            add_mate(FAR, out, sends, h)
            copies.append(rcopy(sib.at[FAR, out, :, span[h]], far.at[out, :, span[h]], f_send.at[out, h], f_recv.at[out, h], target))
            copies[-1].start()
        return copies

    gather_hot((RIGHT, LEFT))
    load_u.wait()
    gather_rows((RIGHT, LEFT), u_v, ureq, 0, n_wide)
    x_right.wait_recv()
    x_far.start()
    x_mate[LEFT].start()
    d_left.wait_recv()
    d_far.start()
    d_mate[RIGHT].start()
    load_v.wait()
    gather_rows((RIGHT, LEFT), v_v, vreq, 0, n_wide)
    x_mate[LEFT].wait_recv()
    dot_x(LEFT)
    d_mate[RIGHT].wait_recv()
    dot_d(RIGHT)
    for copy in q_pass:
        copy.wait_recv()
    gather_hot((FAR,))
    d_right.wait_recv()
    d_mate[LEFT].start()
    x_left.wait_recv()
    x_mate[RIGHT].start()
    gather_rows((FAR,), u_v, ureq, 0, 1)
    gates_here(LEFT)
    coef(LEFT, 0)
    s_left_y = partial(LEFT, 0)
    gates_here(RIGHT)
    x_mate[RIGHT].wait_recv()
    dot_x(RIGHT)
    coef(RIGHT, 1)
    s_right_d = partial(RIGHT, 1)
    for flip in range(2):
        g_out[flip].wait_recv()
        g_pass[flip].start()
    n_left = send_near(LEFT, 0, s_left_y, left)
    gather_rows((FAR,), u_v, ureq, 1, n_wide)
    n_right = send_near(RIGHT, 1, s_right_d, right)
    gather_rows((FAR,), v_v, vreq, 0, n_wide)
    x_far.wait_recv()
    x_mate[FAR].start()
    d_far.wait_recv()
    d_mate[FAR].start()
    d_mate[LEFT].wait_recv()
    dot_d(LEFT)
    coef(LEFT, 1)
    coef(RIGHT, 0)
    s_right_y = partial(RIGHT, 0)
    s_left_d = partial(LEFT, 1)
    gates_here(FAR)
    x_mate[FAR].wait_recv()
    dot_x(FAR)
    coef(FAR, 0)
    s_far_y = partial(FAR, 0)
    d_mate[FAR].wait_recv()
    dot_d(FAR)
    coef(FAR, 1)
    s_far_d = partial(FAR, 1)
    f_y = send_far(0, s_far_y, right)
    f_d = send_far(1, s_far_d, left)
    gather_hot((OWN,))
    gather_rows((OWN,), u_v, ureq, 0, n_wide)
    gather_rows((OWN,), v_v, vreq, 0, n_wide)
    x_mate[OWN].wait_recv()
    d_mate[OWN].wait_recv()
    gates_here(OWN)
    dot_x(OWN)
    dot_d(OWN)
    coef(OWN, 0)
    coef(OWN, 1)
    s_own = [partial(OWN, 0), partial(OWN, 1)]
    o_x = pltpu.make_async_copy(xa, xall_out, out_sem.at[0])
    o_d = pltpu.make_async_copy(da, dyall_out, out_sem.at[1])
    o_x.start()
    o_d.start()
    for rel in range(4):
        place(rel)
    o_c = pltpu.make_async_copy(ct, ct_out, out_sem.at[2])
    o_w = pltpu.make_async_copy(wt, wt_out, out_sem.at[3])
    o_c.start()
    o_w.start()
    for h in range(HALVES):
        add_mate(RIGHT, 0, s_right_y, h)
        add_mate(LEFT, 1, s_left_d, h)
        add_mate(OWN, 0, s_own[0], h)
        add_mate(OWN, 1, s_own[1], h)
    for h in range(HALVES):
        for out, copies in enumerate((n_left, n_right)):
            copies[h].wait_recv()
            own_out[out, :, early[h]] = sib[OWN, out, :, early[h]] + near[out, :, early[h]]
    own_out[:, :, cut:width] = sib[OWN, :, :, cut:width]
    y_next[:, width:width + LATE] = sib[RIGHT, 1, :, cut:width]
    dx_next[:, width:width + LATE] = sib[LEFT, 0, :, cut:width]
    for h in range(HALVES):
        for out, copies, rel, dst in ((0, f_y, RIGHT, y_next), (1, f_d, LEFT, dx_next)):
            copies[h].wait_recv()
            dst[:, span[h]] = sib[rel, out, :, span[h]] + far[out, :, span[h]]
    for key in peers:
        q_copies[key].wait_send()
        g_copies[key].wait_send()
    for copy in (*q_pass, *g_out, *g_pass, x_right, d_left, d_right, x_left, x_far, d_far, *x_mate, *d_mate, *s_far_y, *s_far_d, *s_right_d, *s_right_y, *s_left_y, *s_left_d,
                 *s_own[0], *s_own[1], *n_left, *n_right, *f_y, *f_d):
        copy.wait_send()
    for copy in (o_x, o_d, o_c, o_w):
        copy.wait()


def grad_kernel(ct_ref, wt_ref, xall_ref, dyall_ref, gu_ref, gv_ref):
    width = gu_ref.shape[1]
    for step in range(width // WIDE):
        cols = pl.ds(step * WIDE, WIDE)
        gu_ref[:, cols] = jnp.dot(ct_ref[...], xall_ref[:, cols], preferred_element_type=F32).astype(BF16)
        gv_ref[:, cols] = jnp.dot(wt_ref[...], dyall_ref[:, cols], preferred_element_type=F32).astype(BF16)


def solution(mesh):
    n_dev = mesh.shape['ep']
    tok_spec = P(('dp', 'ep'))
    table_spec = P('ep')
    vmem = pl.BlockSpec(memory_space=pltpu.VMEM)
    hbm = pl.BlockSpec(memory_space=pl.ANY)
    dma = pltpu.SemaphoreType.DMA
    sds = jax.ShapeDtypeStruct

    def per_device(tokens, slot_ids, request_rows, gate_vals, grad_out, up_local, down_local):
        n_tok, width = tokens.shape
        n_rows = up_local.shape[0]
        n_req = request_rows.shape[2]
        sel = slot_ids.shape[1] * slot_ids.shape[2]
        n_all = n_dev * n_tok
        y_next, dx_next, own, xall, dyall, ct, wt = pl.pallas_call(
            exchange_kernel,
            name='exchange',
            out_shape=(pltpu.VMEM((n_tok, width + LATE), F32), pltpu.VMEM((n_tok, width + LATE), F32), pltpu.VMEM((2, n_tok, width), F32),
                       sds((4, 2, n_tok, width), BF16), sds((4, 2, n_tok, width), BF16), sds((n_rows, n_all), BF16), sds((n_rows, n_all), BF16)),
            in_specs=[hbm] * 7,
            out_specs=(vmem,) * 3 + (hbm,) * 4,
            scratch_shapes=[
                pltpu.VMEM((n_rows, width), BF16), pltpu.VMEM((n_rows, width), BF16),
                pltpu.VMEM((n_dev * n_req, width), BF16), pltpu.VMEM((n_dev * n_req, width), BF16),
                pltpu.VMEM((4 * n_req, n_rows), BF16),
                pltpu.VMEM((4, 2, n_tok, width), BF16), pltpu.VMEM((4, 2, n_tok, width), BF16),
                pltpu.VMEM((4, 2, n_tok, n_req), F32), pltpu.VMEM((4, 2, n_dev, n_req), jnp.int32), pltpu.VMEM((2, n_tok, n_req), F32),
                pltpu.VMEM((sel, n_tok), jnp.int32), pltpu.VMEM((sel, n_tok), F32), pltpu.VMEM((n_tok, sel), jnp.int32), pltpu.VMEM((n_tok, sel), F32),
                pltpu.VMEM((n_tok * n_dev, n_req), F32), pltpu.VMEM((n_dev, n_tok, n_req), F32),
                pltpu.VMEM((4, 2 * n_tok, 2 * n_req), F32), pltpu.VMEM((4, 2 * n_tok, 2 * n_req), F32), pltpu.VMEM((4, 4 * n_tok, 2 * n_req), BF16), pltpu.VMEM((n_rows, n_all), BF16), pltpu.VMEM((n_rows, n_all), BF16),
                pltpu.VMEM((4, 2, 2 * n_tok, width), F32), pltpu.VMEM((4, 2, n_tok, width), F32),
                pltpu.VMEM((2, n_tok, width - LATE), F32), pltpu.VMEM((2, n_tok, width), F32),
                dma((7,)), dma((4,)), dma((7,)), dma((7,)), dma((9,)), dma((9,)), dma((6,)), dma((6,)), dma((4, 2)), dma((4, 2)),
                dma((4, 2, HALVES)), dma((4, 2, HALVES)), dma((2, HALVES)), dma((2, HALVES)), dma((2, HALVES)), dma((2, HALVES)),
            ],
            compiler_params=pltpu.CompilerParams(collective_id=0, has_side_effects=True, vmem_limit_bytes=54 * 2 ** 20),
            cost_estimate=pl.CostEstimate(flops=4 * n_dev * n_req * n_rows * width, bytes_accessed=6 * n_rows * width, transcendentals=0),
        )(tokens, grad_out, slot_ids.reshape(n_tok, sel).T, gate_vals.reshape(n_tok, sel).T, request_rows[0], up_local, down_local)

        up_chip = [(d, (d + 2) % n_dev) for d in range(n_dev)]
        down_chip = [(d, (d - 2) % n_dev) for d in range(n_dev)]
        y_last = lax.ppermute(y_next, 'ep', up_chip)
        dx_last = lax.ppermute(dx_next, 'ep', down_chip)

        blk = min(512, n_rows)
        row_spec = lambda cols: pl.BlockSpec((blk, cols), lambda i: (i, 0))
        full_spec = pl.BlockSpec((n_all, width), lambda i: (0, 0))
        grad_up, grad_down = pl.pallas_call(
            grad_kernel,
            name='table_grads',
            out_shape=(sds((n_rows, width), BF16),) * 2,
            grid=(n_rows // blk,),
            in_specs=[row_spec(n_all), row_spec(n_all), full_spec, full_spec],
            out_specs=(row_spec(width),) * 2,
            compiler_params=pltpu.CompilerParams(vmem_limit_bytes=60 * 2 ** 20),
            cost_estimate=pl.CostEstimate(flops=4 * n_rows * n_all * width, bytes_accessed=4 * (n_rows + n_all) * width, transcendentals=0),
        )(ct, wt, xall.reshape(n_all, width), dyall.reshape(n_all, width))
        rest = lambda a: jnp.pad(a[:, width:], ((0, 0), (width - LATE, 0)))
        y = own[0] + y_last[:, :width] + rest(dx_last)
        dx = own[1] + dx_last[:, :width] + rest(y_last)
        return y.astype(BF16), dx.astype(BF16), grad_up, grad_down

    return jax.shard_map(per_device, mesh=mesh, in_specs=(tok_spec, tok_spec, tok_spec, tok_spec, tok_spec, table_spec, table_spec), out_specs=(tok_spec, tok_spec, tok_spec, tok_spec), check_vma=False)
```

```python
import functools
import math

import jax
import jax.numpy as jnp
from jax import lax
from jax.experimental import pallas as pl
from jax.experimental.pallas import tpu as pltpu
from jax.sharding import PartitionSpec as P

MESH = pl.DeviceIdType.MESH
F32 = jnp.float32
BF16 = jnp.bfloat16
NT = (((1,), (1,)), ((), ()))
OWN, RIGHT, FAR, LEFT = 0, 1, 2, 3
ORDER = (RIGHT, LEFT, FAR, OWN)
COLS = 512
WIDE = 1024
LATE = 512
HALVES = 1


def gelu_pair(pre_act):
    normal_cdf = 0.5 * (1.0 + lax.erf(pre_act * (2.0 ** -0.5)))
    normal_pdf = jnp.exp(-0.5 * pre_act * pre_act) * ((2.0 * math.pi) ** -0.5)
    return pre_act * normal_cdf, normal_cdf + pre_act * normal_pdf


def exchange_kernel(x_hbm, dy_hbm, slot_hbm, gate_hbm, req_hbm, u_hbm, v_hbm,
                    y_next, dx_next, own_out, xall_out, dyall_out, ct_out, wt_out,
                    u_v, v_v, ureq, vreq, onehot, xa, da, gall, qall, gpass, slot_in, gate_in, slots, gates, gmix, gloc, dots_x, dots_d, wc, ct, wt, part, sib, near, far,
                    load_sem, out_sem, q_send, q_recv, g_send, g_recv, ax_send, ax_recv, d2d_send, d2d_recv,
                    p_send, p_recv, n_send, n_recv, f_send, f_recv):
    n_dev, n_req = req_hbm.shape
    n_chip = n_dev // 2
    n_tok, width = x_hbm.shape
    n_rows = u_v.shape[0]
    shift = n_req.bit_length() - 1
    me = lax.axis_index('ep')
    core = lax.rem(me, 2)
    chip = me // 2
    other = 1 - core

    def dev(rel, which):
        return lax.rem(chip + rel, n_chip) * 2 + which

    right, left, mate = dev(RIGHT, core), dev(LEFT, core), dev(OWN, other)
    peers = [(rel, flip) for rel in (OWN, RIGHT, LEFT) for flip in range(2) if (rel, flip) != (OWN, 0)]

    def peer_core(flip):
        return core if flip == 0 else other

    barrier = pltpu.get_barrier_semaphore()
    for rel, flip in peers:
        pl.semaphore_signal(barrier, inc=1, device_id={'ep': dev(rel, peer_core(flip))}, device_id_type=MESH)

    load_x = pltpu.make_async_copy(x_hbm, xa.at[OWN, core], load_sem.at[0])
    load_d = pltpu.make_async_copy(dy_hbm, da.at[OWN, core], load_sem.at[1])
    load_q = pltpu.make_async_copy(req_hbm, qall.at[OWN, core], load_sem.at[2])
    load_s = pltpu.make_async_copy(slot_hbm, slot_in, load_sem.at[3])
    load_g = pltpu.make_async_copy(gate_hbm, gate_in, load_sem.at[4])
    load_u = pltpu.make_async_copy(u_hbm, u_v, load_sem.at[5])
    load_v = pltpu.make_async_copy(v_hbm, v_v, load_sem.at[6])
    for load in (load_q, load_x, load_d, load_s, load_g, load_u, load_v):
        load.start()

    def rcopy(src, dst, s_sem, r_sem, target):
        return pltpu.make_async_remote_copy(src_ref=src, dst_ref=dst, send_sem=s_sem, recv_sem=r_sem, device_id={'ep': target}, device_id_type=MESH)

    q_copies, g_copies = {}, {}
    for n, (rel, flip) in enumerate(peers):
        back = (4 - rel) % 4
        target = dev(rel, peer_core(flip))
        q_copies[rel, flip] = rcopy(qall.at[OWN, core], qall.at[back, core], q_send.at[n], q_recv.at[n], target)
        g_copies[rel, flip] = rcopy(gloc.at[target], gall.at[back, core], g_send.at[n], g_recv.at[n], target)
    q_pass = [rcopy(qall.at[LEFT, core], qall.at[FAR, core], q_send.at[5 + flip], q_recv.at[5 + flip], dev(RIGHT, peer_core(flip))) for flip in range(2)]
    g_out = [rcopy(gloc.at[dev(FAR, peer_core(flip))], gpass.at[flip], g_send.at[5 + flip], g_recv.at[5 + flip], (right, left)[flip]) for flip in range(2)]
    g_pass = [rcopy(gpass.at[flip], gall.at[FAR, core], g_send.at[7 + flip], g_recv.at[7 + flip], dev((RIGHT, LEFT)[flip], peer_core(flip))) for flip in range(2)]
    x_right = rcopy(xa.at[OWN, core], xa.at[LEFT, core], ax_send.at[0], ax_recv.at[0], right)
    d_left = rcopy(da.at[OWN, core], da.at[RIGHT, core], ax_send.at[1], ax_recv.at[1], left)
    d_right = rcopy(da.at[OWN, core], da.at[LEFT, core], ax_send.at[2], ax_recv.at[2], right)
    x_left = rcopy(xa.at[OWN, core], xa.at[RIGHT, core], ax_send.at[3], ax_recv.at[3], left)
    x_far = rcopy(xa.at[LEFT, core], xa.at[FAR, core], ax_send.at[4], ax_recv.at[4], right)
    d_far = rcopy(da.at[RIGHT, core], da.at[FAR, core], ax_send.at[5], ax_recv.at[5], left)
    x_mate = [rcopy(xa.at[rel, core], xa.at[rel, core], d2d_send.at[rel, 0], d2d_recv.at[rel, 0], mate) for rel in range(4)]
    d_mate = [rcopy(da.at[rel, core], da.at[rel, core], d2d_send.at[rel, 1], d2d_recv.at[rel, 1], mate) for rel in range(4)]

    load_q.wait()
    load_x.wait()
    load_d.wait()
    pl.semaphore_wait(barrier, len(peers))
    for key in peers:
        q_copies[key].start()
    x_right.start()
    d_left.start()
    x_mate[OWN].start()
    d_mate[OWN].start()
    load_s.wait()
    load_g.wait()
    slots[...] = jnp.transpose(slot_in[...].astype(F32)).astype(jnp.int32)
    gates[...] = jnp.transpose(gate_in[...])

    own_iota = lax.broadcasted_iota(jnp.int32, (n_dev, n_req), 0)
    sub_iota = lax.broadcasted_iota(jnp.int32, (n_req, n_req), 0)

    def gate_step(step, carry):
        base = pl.multiple_of(step * 8, 8)
        s_blk = slots[pl.ds(base, 8), :]
        g_blk = gates[pl.ds(base, 8), :]
        for j in range(8):
            s_row = s_blk[j:j + 1, :]
            g_row = g_blk[j:j + 1, :]
            spread = jnp.where(own_iota == (s_row >> shift), g_row, 0.0)
            hi = spread.astype(BF16).astype(F32)
            rest = spread - hi
            mid = rest.astype(BF16).astype(F32)
            lo = rest - mid
            lhs = jnp.concatenate([hi, mid, lo], axis=0).astype(BF16)
            hot = jnp.where(sub_iota == (s_row & (n_req - 1)), 1.0, 0.0).astype(BF16)
            res = lax.dot_general(lhs, hot, NT, preferred_element_type=F32)
            start = pl.multiple_of((base + j) * n_dev, n_dev)
            gmix[pl.ds(start, n_dev), :] = res[0:n_dev] + res[n_dev:2 * n_dev] + res[2 * n_dev:3 * n_dev]
        return carry

    lax.fori_loop(0, n_tok // 8, gate_step, 0)
    for o in range(n_dev):
        gloc[o] = gmix[pl.ds(o, n_tok, stride=n_dev), :]
    for key in peers:
        q_copies[key].wait_recv()
    for copy in q_pass:
        copy.start()
    d_right.start()
    x_left.start()
    for copy in g_out:
        copy.start()
    for key in peers:
        g_copies[key].start()
    gall[OWN, core] = gloc[me]

    lane_iota = lax.broadcasted_iota(jnp.int32, (n_req, n_req), 1).astype(F32)

    def lists(rel):
        return [qall[rel, which, pl.ds(me, 1), :] for which in range(2)]

    def gather_hot(rels):
        rows = [r.astype(F32) for rel in rels for r in lists(rel)]
        stack = jnp.broadcast_to(rows[0], (n_req, n_req))
        for n in range(1, len(rows)):
            stack = jnp.where(sub_iota == n, rows[n], stack)
        cols = jnp.transpose(stack)
        for n in range(len(rows)):
            col = jnp.broadcast_to(cols[:, n:n + 1], (n_req, n_req))
            for blk in range(n_rows // n_req):
                onehot[pl.ds(n * n_req, n_req), pl.ds(blk * n_req, n_req)] = jnp.where(col - blk * n_req == lane_iota, 1.0, 0.0).astype(BF16)

    def gather_rows(rels, src, dst, first, last):
        size = len(rels) * 2 * n_req
        base = ORDER.index(rels[0]) * 2 * n_req

        def body(step, carry):
            cols = pl.ds(pl.multiple_of(step * WIDE, WIDE), WIDE)
            dst[base:base + size, cols] = jnp.dot(onehot[0:size, :], src[:, cols], preferred_element_type=F32).astype(BF16)
            return carry

        lax.fori_loop(first, last, body, 0)

    def rows_of(table, rel, cols=slice(None)):
        base = ORDER.index(rel) * 2 * n_req
        return table[base:base + 2 * n_req, cols]

    zeros = jnp.zeros((n_tok, n_req), BF16)

    def tokens_of(buf, rel):
        return buf[rel].reshape(2 * n_tok, width)

    def dot_x(rel):
        dots_x[rel] = lax.dot_general(tokens_of(xa, rel), rows_of(ureq, rel), NT, preferred_element_type=F32)

    def dot_d(rel):
        dots_d[rel] = lax.dot_general(tokens_of(da, rel), rows_of(vreq, rel), NT, preferred_element_type=F32)

    def gates_here(rel):
        for flip in range(2):
            if rel == FAR:
                g_pass[flip].wait_recv()
            elif (rel, flip) != (OWN, 0):
                g_copies[(4 - rel) % 4, flip].wait_recv()

    def coef(rel, out):
        for which in range(2):
            toks, slot = pl.ds(which * n_tok, n_tok), pl.ds(which * n_req, n_req)
            act, slope = gelu_pair(dots_x[rel, toks, slot])
            value = gall[rel, which] * (act if out == 0 else slope)
            if out == 1:
                value = value * dots_d[rel, toks, slot]
            row = pl.ds((out * 2 + which) * n_tok, n_tok)
            wc[rel, row, slot] = value.astype(BF16)
            wc[rel, row, pl.ds((1 - which) * n_req, n_req)] = zeros

    theirs = pl.ds(pl.multiple_of(other * n_tok, n_tok), n_tok)
    mine = pl.ds(pl.multiple_of(core * n_tok, n_tok), n_tok)

    span = [pl.ds(h * width // HALVES, width // HALVES) for h in range(HALVES)]

    def partial(rel, out):
        table = vreq if out == 0 else ureq
        sends = []
        for h, cols in enumerate(span):
            part[rel, out, :, cols] = jnp.dot(wc[rel, out * 2 * n_tok:(out + 1) * 2 * n_tok, :], rows_of(table, rel, cols), preferred_element_type=F32)
            sends.append(rcopy(part.at[rel, out, theirs, cols], sib.at[rel, out, :, cols], p_send.at[rel, out, h], p_recv.at[rel, out, h], mate))
            sends[-1].start()
        return sends

    def add_mate(rel, out, sends, h):
        sends[h].wait_recv()
        sib[rel, out, :, span[h]] = sib[rel, out, :, span[h]] + part[rel, out, mine, span[h]]

    def place(rel):
        rows = jnp.concatenate(lists(rel), axis=1)
        blk = n_rows // 2

        def body(step, carry):
            base = pl.multiple_of(step * blk, blk)
            hot = jnp.where(lax.broadcasted_iota(jnp.int32, (blk, 2 * n_req), 0) + base == rows, 1.0, 0.0).astype(BF16)
            coef = lax.dot_general(hot, wc[rel], NT, preferred_element_type=F32).astype(BF16)
            wt[pl.ds(base, blk), rel * 2 * n_tok:(rel + 1) * 2 * n_tok] = coef[:, :2 * n_tok]
            ct[pl.ds(base, blk), rel * 2 * n_tok:(rel + 1) * 2 * n_tok] = coef[:, 2 * n_tok:]
            return carry

        lax.fori_loop(0, n_rows // blk, body, 0)

    n_wide = width // WIDE
    cut = width - LATE
    part_half = width // HALVES
    early = [pl.ds(h * part_half, min(part_half, cut - h * part_half)) for h in range(HALVES)]

    def send_near(rel, out, sends, target):
        copies = []
        for h in range(HALVES):
            add_mate(rel, out, sends, h)
            copies.append(rcopy(sib.at[rel, out, :, early[h]], near.at[out, :, early[h]], n_send.at[out, h], n_recv.at[out, h], target))
            copies[-1].start()
        return copies

    def send_far(out, sends, target):
        copies = []
        for h in range(HALVES):
            add_mate(FAR, out, sends, h)
            copies.append(rcopy(sib.at[FAR, out, :, span[h]], far.at[out, :, span[h]], f_send.at[out, h], f_recv.at[out, h], target))
            copies[-1].start()
        return copies

    gather_hot((RIGHT, LEFT))
    load_u.wait()
    gather_rows((RIGHT, LEFT), u_v, ureq, 0, n_wide)
    x_right.wait_recv()
    x_far.start()
    x_mate[LEFT].start()
    d_left.wait_recv()
    d_far.start()
    d_mate[RIGHT].start()
    load_v.wait()
    gather_rows((RIGHT, LEFT), v_v, vreq, 0, n_wide)
    x_mate[LEFT].wait_recv()
    dot_x(LEFT)
    d_mate[RIGHT].wait_recv()
    dot_d(RIGHT)
    for copy in q_pass:
        copy.wait_recv()
    gather_hot((FAR,))
    d_right.wait_recv()
    d_mate[LEFT].start()
    x_left.wait_recv()
    x_mate[RIGHT].start()
    gather_rows((FAR,), u_v, ureq, 0, 1)
    gates_here(LEFT)
    coef(LEFT, 0)
    s_left_y = partial(LEFT, 0)
    gates_here(RIGHT)
    x_mate[RIGHT].wait_recv()
    dot_x(RIGHT)
    coef(RIGHT, 1)
    s_right_d = partial(RIGHT, 1)
    for flip in range(2):
        g_out[flip].wait_recv()
        g_pass[flip].start()
    n_left = send_near(LEFT, 0, s_left_y, left)
    gather_rows((FAR,), u_v, ureq, 1, n_wide)
    n_right = send_near(RIGHT, 1, s_right_d, right)
    gather_rows((FAR,), v_v, vreq, 0, n_wide)
    x_far.wait_recv()
    x_mate[FAR].start()
    d_far.wait_recv()
    d_mate[FAR].start()
    d_mate[LEFT].wait_recv()
    dot_d(LEFT)
    coef(LEFT, 1)
    coef(RIGHT, 0)
    s_right_y = partial(RIGHT, 0)
    s_left_d = partial(LEFT, 1)
    gates_here(FAR)
    x_mate[FAR].wait_recv()
    dot_x(FAR)
    coef(FAR, 0)
    s_far_y = partial(FAR, 0)
    d_mate[FAR].wait_recv()
    dot_d(FAR)
    coef(FAR, 1)
    s_far_d = partial(FAR, 1)
    f_y = send_far(0, s_far_y, right)
    f_d = send_far(1, s_far_d, left)
    gather_hot((OWN,))
    gather_rows((OWN,), u_v, ureq, 0, n_wide)
    gather_rows((OWN,), v_v, vreq, 0, n_wide)
    x_mate[OWN].wait_recv()
    d_mate[OWN].wait_recv()
    gates_here(OWN)
    dot_x(OWN)
    dot_d(OWN)
    coef(OWN, 0)
    coef(OWN, 1)
    s_own = [partial(OWN, 0), partial(OWN, 1)]
    o_x = pltpu.make_async_copy(xa, xall_out, out_sem.at[0])
    o_d = pltpu.make_async_copy(da, dyall_out, out_sem.at[1])
    o_x.start()
    o_d.start()
    for rel in range(4):
        place(rel)
    o_c = pltpu.make_async_copy(ct, ct_out, out_sem.at[2])
    o_w = pltpu.make_async_copy(wt, wt_out, out_sem.at[3])
    o_c.start()
    o_w.start()
    for h in range(HALVES):
        add_mate(RIGHT, 0, s_right_y, h)
        add_mate(LEFT, 1, s_left_d, h)
        add_mate(OWN, 0, s_own[0], h)
        add_mate(OWN, 1, s_own[1], h)
    for h in range(HALVES):
        for out, copies in enumerate((n_left, n_right)):
            copies[h].wait_recv()
            own_out[out, :, early[h]] = sib[OWN, out, :, early[h]] + near[out, :, early[h]]
    own_out[:, :, cut:width] = sib[OWN, :, :, cut:width]
    y_next[:, width:width + LATE] = sib[RIGHT, 1, :, cut:width]
    dx_next[:, width:width + LATE] = sib[LEFT, 0, :, cut:width]
    for h in range(HALVES):
        for out, copies, rel, dst in ((0, f_y, RIGHT, y_next), (1, f_d, LEFT, dx_next)):
            copies[h].wait_recv()
            dst[:, span[h]] = sib[rel, out, :, span[h]] + far[out, :, span[h]]
    for key in peers:
        q_copies[key].wait_send()
        g_copies[key].wait_send()
    for copy in (*q_pass, *g_out, *g_pass, x_right, d_left, d_right, x_left, x_far, d_far, *x_mate, *d_mate, *s_far_y, *s_far_d, *s_right_d, *s_right_y, *s_left_y, *s_left_d,
                 *s_own[0], *s_own[1], *n_left, *n_right, *f_y, *f_d):
        copy.wait_send()
    for copy in (o_x, o_d, o_c, o_w):
        copy.wait()


def grad_kernel(ct_ref, wt_ref, xall_ref, dyall_ref, gu_ref, gv_ref):
    width = gu_ref.shape[1]
    for step in range(width // WIDE):
        cols = pl.ds(step * WIDE, WIDE)
        gu_ref[:, cols] = jnp.dot(ct_ref[...], xall_ref[:, cols], preferred_element_type=F32).astype(BF16)
        gv_ref[:, cols] = jnp.dot(wt_ref[...], dyall_ref[:, cols], preferred_element_type=F32).astype(BF16)


def solution(mesh):
    n_dev = mesh.shape['ep']
    tok_spec = P(('dp', 'ep'))
    table_spec = P('ep')
    vmem = pl.BlockSpec(memory_space=pltpu.VMEM)
    hbm = pl.BlockSpec(memory_space=pl.ANY)
    dma = pltpu.SemaphoreType.DMA
    sds = jax.ShapeDtypeStruct

    def per_device(tokens, slot_ids, request_rows, gate_vals, grad_out, up_local, down_local):
        n_tok, width = tokens.shape
        n_rows = up_local.shape[0]
        n_req = request_rows.shape[2]
        sel = slot_ids.shape[1] * slot_ids.shape[2]
        n_all = n_dev * n_tok
        y_next, dx_next, own, xall, dyall, ct, wt = pl.pallas_call(
            exchange_kernel,
            name='exchange',
            out_shape=(pltpu.VMEM((n_tok, width + LATE), F32), pltpu.VMEM((n_tok, width + LATE), F32), pltpu.VMEM((2, n_tok, width), F32),
                       sds((4, 2, n_tok, width), BF16), sds((4, 2, n_tok, width), BF16), sds((n_rows, n_all), BF16), sds((n_rows, n_all), BF16)),
            in_specs=[hbm] * 7,
            out_specs=(vmem,) * 3 + (hbm,) * 4,
            scratch_shapes=[
                pltpu.VMEM((n_rows, width), BF16), pltpu.VMEM((n_rows, width), BF16),
                pltpu.VMEM((n_dev * n_req, width), BF16), pltpu.VMEM((n_dev * n_req, width), BF16),
                pltpu.VMEM((4 * n_req, n_rows), BF16),
                pltpu.VMEM((4, 2, n_tok, width), BF16), pltpu.VMEM((4, 2, n_tok, width), BF16),
                pltpu.VMEM((4, 2, n_tok, n_req), F32), pltpu.VMEM((4, 2, n_dev, n_req), jnp.int32), pltpu.VMEM((2, n_tok, n_req), F32),
                pltpu.VMEM((sel, n_tok), jnp.int32), pltpu.VMEM((sel, n_tok), F32), pltpu.VMEM((n_tok, sel), jnp.int32), pltpu.VMEM((n_tok, sel), F32),
                pltpu.VMEM((n_tok * n_dev, n_req), F32), pltpu.VMEM((n_dev, n_tok, n_req), F32),
                pltpu.VMEM((4, 2 * n_tok, 2 * n_req), F32), pltpu.VMEM((4, 2 * n_tok, 2 * n_req), F32), pltpu.VMEM((4, 4 * n_tok, 2 * n_req), BF16), pltpu.VMEM((n_rows, n_all), BF16), pltpu.VMEM((n_rows, n_all), BF16),
                pltpu.VMEM((4, 2, 2 * n_tok, width), F32), pltpu.VMEM((4, 2, n_tok, width), F32),
                pltpu.VMEM((2, n_tok, width - LATE), F32), pltpu.VMEM((2, n_tok, width), F32),
                dma((7,)), dma((4,)), dma((7,)), dma((7,)), dma((9,)), dma((9,)), dma((6,)), dma((6,)), dma((4, 2)), dma((4, 2)),
                dma((4, 2, HALVES)), dma((4, 2, HALVES)), dma((2, HALVES)), dma((2, HALVES)), dma((2, HALVES)), dma((2, HALVES)),
            ],
            compiler_params=pltpu.CompilerParams(collective_id=0, has_side_effects=True, vmem_limit_bytes=54 * 2 ** 20),
            cost_estimate=pl.CostEstimate(flops=4 * n_dev * n_req * n_rows * width, bytes_accessed=6 * n_rows * width, transcendentals=0),
        )(tokens, grad_out, slot_ids.reshape(n_tok, sel).T, gate_vals.reshape(n_tok, sel).T, request_rows[0], up_local, down_local)

        up_chip = [(d, (d + 2) % n_dev) for d in range(n_dev)]
        down_chip = [(d, (d - 2) % n_dev) for d in range(n_dev)]
        y_last = lax.ppermute(y_next, 'ep', up_chip)
        dx_last = lax.ppermute(dx_next, 'ep', down_chip)

        blk = min(512, n_rows)
        row_spec = lambda cols: pl.BlockSpec((blk, cols), lambda i: (i, 0))
        full_spec = pl.BlockSpec((n_all, width), lambda i: (0, 0))
        grad_up, grad_down = pl.pallas_call(
            grad_kernel,
            name='table_grads',
            out_shape=(sds((n_rows, width), BF16),) * 2,
            grid=(n_rows // blk,),
            in_specs=[row_spec(n_all), row_spec(n_all), full_spec, full_spec],
            out_specs=(row_spec(width),) * 2,
            compiler_params=pltpu.CompilerParams(vmem_limit_bytes=60 * 2 ** 20),
            cost_estimate=pl.CostEstimate(flops=4 * n_rows * n_all * width, bytes_accessed=4 * (n_rows + n_all) * width, transcendentals=0),
        )(ct, wt, xall.reshape(n_all, width), dyall.reshape(n_all, width))
        rest = lambda a: jnp.pad(a[:, width:], ((0, 0), (width - LATE, 0)))
        y = own[0] + y_last[:, :width] + rest(dx_last)
        dx = own[1] + dx_last[:, :width] + rest(y_last)
        return y.astype(BF16), dx.astype(BF16), grad_up, grad_down

    return jax.shard_map(per_device, mesh=mesh, in_specs=(tok_spec, tok_spec, tok_spec, tok_spec, tok_spec, table_spec, table_spec), out_specs=(tok_spec, tok_spec, tok_spec, tok_spec), check_vma=False)
```
